32 devices in a mesh: seq: 8 (over z, y), batch: 4 (over x, core).
Axes of the slice: x: 2, y: 2, z: 4, core: 2. Of those that a mesh axis runs over, the one named last changes fastest.
Arguments:
- tokens: bfloat16 [4, 8192, 1024], P('batch', 'seq'), may hold values from -6 to 6
- logits: bfloat16 [4, 8192, 256], P('batch', 'seq'), may hold values from -160 to 160
- slot_grad: bfloat16 [4, 256, 1024], P('batch', 'seq'), may hold values from -6 to 6
- phi_param: bfloat16 [1024, 256], P('seq'), may hold values from -0.1875 to 0.1875
Outputs:
- token_grad: bfloat16 [4, 8192, 1024], P('batch', 'seq')
- phi_grad: float32 [1024, 256], P('seq')
The draws below stay inside these ranges and needn't reach their ends.
All inputs are finite; a program needn't handle non-finite values.
Results may differ from the reference program's by a relative error of at most 0.0049.
Values may be sent and summed in bfloat16 or wider, within the bound.
A program may use at most 64 MiB of HBM per device.

```python
import jax
import jax.numpy as jnp
from jax import lax

D = 1024
SLOTS = 256
TOK_DEV = 1024
SEQ_TOKENS = 8192
BATCH = 4


def draw_logits(key, part):
    key_base = jax.random.fold_in(key, 0)
    key_tilt = jax.random.fold_in(key, 1)
    key_offset = jax.random.fold_in(key, 3)
    block_count = SEQ_TOKENS // TOK_DEV
    values = jnp.clip(jax.random.normal(key_base, (BATCH, SEQ_TOKENS, SLOTS), jnp.float32), -6.0, 6.0) * 1.5
    block_tilt = jax.random.uniform(key_tilt, (BATCH, block_count, 1, SLOTS), jnp.float32, -2.0, 2.0)
    values = (values.reshape(BATCH, block_count, TOK_DEV, SLOTS) + block_tilt).reshape(BATCH, SEQ_TOKENS, SLOTS)
    offset = jax.random.uniform(key_offset, (SLOTS,), jnp.float32, -3.0, 3.0)
    values = values + offset
    return jnp.clip(values, -160.0, 160.0).astype(jnp.bfloat16)


def spiked(entries, key, source, target, parts, factor):
    def block_of(axis_at):
        return (jnp.arange(entries.shape[axis_at]) // (entries.shape[axis_at] // parts)).reshape((-1,) + (1,) * (entries.ndim - 1 - axis_at))

    one_side = jax.random.permutation(key, parts)[block_of(target)]
    other_side = (block_of(target) + parts // 2) % parts
    return jnp.where((block_of(source) == one_side) | (block_of(source) == other_side), factor * entries, entries)


def steps_of(rng, shape, shards, smallest, top_value):
    level = 1.0
    for position, parts in shards:
        steps = jax.random.uniform(jax.random.fold_in(jax.random.fold_in(rng, 6), position), (parts,), jnp.float32, smallest / len(shards), top_value / len(shards))
        level = level * jnp.repeat(jnp.exp(steps), shape[position] // parts).reshape((-1,) + (1,) * (len(shape) - 1 - position))
    return level


def scatter_about(rng, dims, spread, most, cuts=(), kind=jnp.bfloat16):
    drawn = spread * jax.random.normal(rng, dims, jnp.float32)
    if cuts:
        drawn = drawn * steps_of(rng, dims, cuts, -0.22, 0.18)
    return jnp.clip(drawn, -most, most).astype(kind)


def gaussian_with(rng, extent, deviation, bound, pieces, heavy, held_as=jnp.bfloat16):
    drawn = deviation * jax.random.normal(rng, extent, jnp.float32)
    if pieces:
        drawn = drawn * steps_of(rng, extent, pieces, -0.22, 0.18)
    return jnp.clip(spiked(drawn, jax.random.fold_in(rng, 3), *heavy), -bound, bound).astype(held_as)


def setup_inputs(seed: int = 0) -> dict:
    arg_keys = jax.random.split(jax.random.key(seed), 5)
    tokens = gaussian_with(arg_keys[0], (BATCH, SEQ_TOKENS, D), 1.0, 6.0, ((0, 4), (1, 8)), (1, 2, 8, 2.0))
    logits = draw_logits(jax.random.fold_in(arg_keys[4], 71), 0)
    slot_grad = scatter_about(arg_keys[2], (BATCH, SLOTS, D), 1.0, 6.0, ((0, 4), (1, 8)))
    phi_param = scatter_about(arg_keys[3], (D, SLOTS), D ** -0.5, 0.1875, ((0, 8),))
    return dict(tokens=tokens, logits=logits, slot_grad=slot_grad, phi_param=phi_param)


def reference(tokens, logits, slot_grad, phi_param):
    grad_scale = float(SEQ_TOKENS // 16)
    phi_grad = jnp.zeros((D, SLOTS), jnp.float32)
    results = []
    for seq_index in range(BATCH):
        inputs = tokens[seq_index]
        scores = logits[seq_index].astype(jnp.float32)
        upstream = slot_grad[seq_index]
        col_peak = jnp.max(scores, axis=0, keepdims=True)
        raw_weights = jnp.exp(scores - col_peak)
        col_total = jnp.sum(raw_weights, axis=0, keepdims=True)
        dispatch = raw_weights / col_total
        weight_grad = lax.dot_general(inputs, upstream, (((1,), (1,)), ((), ())), preferred_element_type=jnp.float32)
        col_dot = jnp.sum(dispatch * weight_grad, axis=0, keepdims=True)
        logit_grad = (dispatch * (weight_grad - col_dot)).astype(jnp.bfloat16)
        dispatch_low = dispatch.astype(jnp.bfloat16)
        token_sum = jnp.dot(dispatch_low, upstream, preferred_element_type=jnp.float32)
        token_sum = token_sum + lax.dot_general(logit_grad, phi_param, (((1,), (1,)), ((), ())), preferred_element_type=jnp.float32)
        results.append((grad_scale * token_sum).astype(jnp.bfloat16))
        phi_grad = phi_grad + lax.dot_general(inputs, logit_grad, (((0,), (0,)), ((), ())), preferred_element_type=jnp.float32)
    return jnp.stack(results), phi_grad
```

```python
import functools

import jax
import jax.numpy as jnp
from jax import lax
from jax.experimental import pallas as pl
from jax.experimental.pallas import tpu as pltpu
from jax.sharding import PartitionSpec as P

MESH = pl.DeviceIdType.MESH
F32 = jnp.float32
BF16 = jnp.bfloat16
PIECES = 2
LAG = 0.5


def fused_kernel(
    n, scale, tok_hbm, log_hbm, slot_hbm, phi_hbm, tok_out, phi_out,
    tok, log, raw, raw_low, wg, gath, phig, ends, dots, gam, disp, lg, tokt,
    mass, mass_in, part, part_low, recv_a, sum_a, low_a, recv_b, sum_b, low_b, recv_c, fin,
    load_sem, ag_send, ag_recv, fw_send, fw_recv, en_send, en_recv, do_send, do_recv, ga_send, ga_recv,
    ph_send, ph_recv, pa_send, pa_recv, m_send, m_recv,
    a_send, a_recv, b_send, b_recv, c_send, c_recv, d_send, d_recv,
):
    me = lax.axis_index("seq")
    bat = lax.axis_index("batch")
    half = n // 2
    place = me // 2
    col = me % 2
    twin = me + 1 - 2 * col
    bat_a = bat + 1 - 2 * (bat % 2)
    bat_b = (bat + 2) % 4
    bat_c = (bat_a + 2) % 4
    keep_a = bat % 2
    keep_b = bat // 2
    mates = ((bat_a, 1 - keep_a, keep_b), (bat_b, keep_a, 1 - keep_b), (bat_c, 1 - keep_a, 1 - keep_b))
    rows = tok.shape[0]
    slots = log.shape[1]
    step = min(256, rows)
    steps = rows // step
    large = 2 * step if rows % (2 * step) == 0 else step
    pieces, span = gath.shape[0], gath.shape[3]
    own = tok.shape[1] // n
    quarter = own // 4
    group = n // 2
    owners = [[j for j in range(n) if (n // 4 <= j < n - n // 4) == bool(g)] for g in range(2)]

    def remote(src, dst, send, recv, seq_at, bat_at):
        return pltpu.make_async_remote_copy(
            src_ref=src, dst_ref=dst, send_sem=send, recv_sem=recv,
            device_id=(seq_at, bat_at), device_id_type=MESH,
        )

    def chunk(i):
        return pl.ds(pl.multiple_of(i * step, step), step)

    def wide(i):
        return pl.ds(pl.multiple_of(i * large, large), large)

    load_slot = [
        pltpu.make_async_copy(slot_hbm.at[:, q * span : (q + 1) * span], gath.at[q, me], load_sem.at[3 + q])
        for q in range(pieces)
    ]
    load_log = pltpu.make_async_copy(log_hbm, log, load_sem.at[0])
    load_phi = pltpu.make_async_copy(phi_hbm.at[keep_a], phig.at[me, keep_a], load_sem.at[1])
    load_tok = pltpu.make_async_copy(tok_hbm, tok, load_sem.at[2])
    for load in load_slot:
        load.start()
    load_log.start()
    load_tok.start()
    load_phi.start()

    barrier = pltpu.get_barrier_semaphore()
    for k in range(1, n):
        pl.semaphore_signal(barrier, inc=1, device_id=((me + k) % n, bat), device_id_type=MESH)
    for other in (bat_a, bat_b, bat_c):
        pl.semaphore_signal(barrier, inc=1, device_id=(me, other), device_id_type=MESH)
    pl.semaphore_wait(barrier, n - 1 + 3)

    def inside(p):
        return (p >= 0) & (p < half)

    def to_twin(p, q):
        shard = gath.at[q, 2 * p + col]
        return remote(shard, shard, fw_send, fw_recv.at[q], twin, bat)

    def along(p, target, q):
        shard = gath.at[q, 2 * p + col]
        return remote(shard, shard, ag_send, ag_recv.at[p, q], 2 * target + col, bat)

    def send_own():
        for q in range(pieces):
            load_slot[q].wait()
            to_twin(place, q).start()
            for dist in range(1, half):
                for sign in (1, -1):
                    @pl.when(inside(place + sign * dist))
                    def _(dist=dist, sign=sign, q=q):
                        along(place, place + sign * dist, q).start()

    def arrive(dist, sign, q):
        p = place + sign * dist

        @pl.when(inside(p))
        def _():
            along(p, p, q).wait_recv()
            to_twin(p, q).start()

    def whole(ref, sem):
        return remote(ref, ref, sem, sem, me, bat_a)

    @pl.when(keep_a == 0)
    def _():
        send_own()

    load_log.wait()

    def peak_step(i, top):
        return jnp.maximum(top, jnp.max(log[chunk(i), :].astype(F32), axis=0, keepdims=True))

    peak = lax.fori_loop(0, steps, peak_step, jnp.full((1, slots), -jnp.inf, F32))

    def exp_step(i, acc):
        values = jnp.exp(log[chunk(i), :].astype(F32) - peak)
        raw[chunk(i), :] = values
        raw_low[chunk(i), :] = values.astype(BF16)
        return acc + jnp.sum(values, axis=0, keepdims=True)

    total = lax.fori_loop(0, steps, exp_step, jnp.zeros((1, slots), F32))
    ends[me, 0:1, :] = peak
    ends[me, 1:2, :] = total
    for k in range(1, n):
        remote(ends.at[me], ends.at[me], en_send, en_recv, (me + k) % n, bat).start()

    @pl.when(keep_a == 1)
    def _():
        send_own()

    load_tok.wait()

    def turn_step(i, carry):
        tokt[:, chunk(i)] = tok[chunk(i), :].T
        return carry

    lax.fori_loop(0, steps, turn_step, 0)

    def terms_of(weights, g, at, put):
        j = owners[g][at]
        terms = jnp.dot(tokt[own * j : own * (j + 2), :], weights[...], preferred_element_type=F32)
        for side in range(2):
            for qa in range(2):
                for qb in range(2):
                    first = own * side + (2 * qa + qb) * quarter
                    put(g, qa, qb, at + side, terms[first : first + quarter, :])

    def put_mass(g, qa, qb, at, block):
        mass[g, qa, qb, at] = block.astype(BF16)


    def mass_task(g, at):
        terms_of(raw_low, g, at, put_mass)
        if at + 2 == group:
            for k, (mate, qa, qb) in enumerate(mates):
                remote(mass.at[g, qa, qb], mass_in.at[k, g], m_send, m_recv, me, mate).start()

    tasks = [(g, at) for g in range(2) for at in range(0, group, 2)]
    coming = sorted((q + LAG * (dist - 1), dist, q) for q in range(pieces) for dist in range(1, half))
    for _, dist, q in coming:
        if tasks:
            mass_task(*tasks.pop(0))
        for sign in (1, -1):
            arrive(dist, sign, q)
    for task in tasks:
        mass_task(*task)

    whole(ends.at[: n - 1], en_recv).wait_recv()
    peaks = ends[:, 0:1, :]
    col_peak = jnp.max(peaks, axis=0)
    col_total = jnp.sum(ends[:, 1:2, :] * jnp.exp(peaks - col_peak), axis=0)
    factor = jnp.exp(peak - col_peak) / col_total

    dot = jnp.zeros((1, slots), F32)
    for q in range(pieces):
        whole(gath.at[q, :half], fw_recv.at[q]).wait_recv()

        def wg_step(i, acc, q=q):
            values = lax.dot_general(
                tok[wide(i), q * span : (q + 1) * span], gath[q].reshape(slots, span),
                (((1,), (1,)), ((), ())), preferred_element_type=F32,
            )
            if q:
                values = values + wg[wide(i), :]
            wg[wide(i), :] = values
            if q == pieces - 1:
                acc = acc + jnp.sum(values * raw[wide(i), :], axis=0, keepdims=True)
            return acc

        dot = lax.fori_loop(0, rows // large, wg_step, dot)

    dots[me] = factor * dot
    for k in range(1, n):
        remote(dots.at[me], dots.at[me], do_send, do_recv, (me + k) % n, bat).start()
    load_phi.wait()
    for k in range(1, n):
        remote(phig.at[me, keep_a], phig.at[me, keep_a], ph_send, ph_recv, (me + k) % n, bat).start()

    center = dot / total

    def center_step(i, carry):
        lg[chunk(i), :] = (raw[chunk(i), :] * factor * (wg[chunk(i), :] - center)).astype(BF16)
        return carry

    lax.fori_loop(0, steps, center_step, 0)

    def put_part(g, qa, qb, at, block):
        part[g, qa, qb, at] = block
        part_low[g, qa, qb, at] = block.astype(BF16)

    moves_a = []
    for g in range(2):
        for at in range(0, group, 2):
            terms_of(lg, g, at, put_part)
        moves_a.append(remote(part_low.at[g, 1 - keep_a], recv_a.at[g], a_send, a_recv.at[g], me, bat_a))
        moves_a[-1].start()
    moves_b = []
    for g in range(2):
        moves_a[g].wait_recv()
        for qb in range(2):
            for at in range(group):
                block = part[g, keep_a, qb, at] + recv_a[g, qb, at].astype(F32)
                sum_a[g, qb, at] = block
                low_a[g, qb, at] = block.astype(BF16)
        moves_b.append(remote(low_a.at[g, 1 - keep_b], recv_b.at[g], b_send, b_recv.at[g], me, bat_b))
        moves_b[-1].start()

    whole(dots.at[: n - 1], do_recv).wait_recv()
    col_dot = jnp.sum(dots[...], axis=0)
    gam[0] = factor * (center - col_dot)
    for k, (mate, _, _) in enumerate(mates):
        remote(gam.at[0], gam.at[1 + k], ga_send, ga_recv, me, mate).start()

    def grad_step(i, carry):
        weights = raw[chunk(i), :] * factor
        grads = weights * (wg[chunk(i), :] - col_dot)
        disp[chunk(i), :] = weights.astype(BF16)
        lg[chunk(i), :] = grads.astype(BF16)
        return carry

    lax.fori_loop(0, steps, grad_step, 0)

    whole(mass_in, m_recv).wait_recv()
    whole(gam.at[1:], ga_recv).wait_recv()

    def share_move(g, at):
        j = owners[g][at]
        return remote(low_b.at[g, at], recv_c.at[me], c_send, c_recv, j, bat)

    for g in range(2):
        moves_b[g].wait_recv()
        for at in range(group):
            block = sum_a[g, keep_b, at] + recv_b[g, at].astype(F32)
            block = block + mass[g, keep_a, keep_b, at].astype(F32) * gam[0]
            for k in range(3):
                block = block + mass_in[k, g, at].astype(F32) * gam[1 + k]
            sum_b[owners[g][at]] = block
            low_b[g, at] = block.astype(BF16)
        for at in range(group):
            @pl.when(me != owners[g][at])
            def _(g=g, at=at):
                share_move(g, at).start()

    whole(phig.at[: n - 1, 0], ph_recv).wait_recv()
    phi_a = remote(phig.at[:, keep_a], phig.at[:, keep_a], pa_send, pa_recv, me, bat_a)
    phi_a.start()
    phi_a.wait_recv()
    phi_full = phig.reshape(n * own, slots)

    def out_step(i, carry):
        for q in range(pieces):
            values = jnp.dot(disp[wide(i), :], gath[q].reshape(slots, span), preferred_element_type=F32)
            values = values + lax.dot_general(
                lg[wide(i), :], phi_full[q * span : (q + 1) * span, :],
                (((1,), (1,)), ((), ())), preferred_element_type=F32,
            )
            tok_out[wide(i), q * span : (q + 1) * span] = (scale * values).astype(BF16)
        return carry

    lax.fori_loop(0, rows // large, out_step, 0)

    share = sum_b[me]
    whole(recv_c.at[: n - 1], c_recv).wait_recv()
    for k in range(1, n):
        share = share + recv_c[(me - k + n) % n].astype(F32)
    mine = 2 * keep_a + keep_b
    fin[mine] = share
    for k, other in enumerate((bat_c, bat_b, bat_a)):
        remote(fin.at[mine], fin.at[mine], d_send, d_recv, me, other).start()
    whole(fin.at[:3], d_recv).wait_recv()
    phi_out[...] = fin[...].reshape(own, slots)

    for ref, sem in (
        (gath.at[:, : half - 1], ag_send), (gath.at[:, :half], fw_send), (ends.at[: n - 1], en_send), (dots.at[: n - 1], do_send),
        (gam.at[1:], ga_send), (phig.at[: n - 1, 0], ph_send), (phig.at[:, 0], pa_send), (mass_in, m_send),
        (recv_a, a_send), (recv_b, b_send), (recv_c.at[: n - 1], c_send), (fin.at[:3], d_send),
    ):
        whole(ref, sem).wait_send()


def fused(n, tokens, logits, slot_grad, phi_param):
    rows, width = tokens.shape
    slots = logits.shape[1]
    own = width // n
    quarter = own // 4
    half = n // 2
    scale = float(n * rows // 16)
    dma = pltpu.SemaphoreType.DMA
    hbm = pl.BlockSpec(memory_space=pltpu.HBM)
    return pl.pallas_call(
        functools.partial(fused_kernel, n, scale),
        out_shape=(
            jax.ShapeDtypeStruct((rows, width), BF16),
            jax.ShapeDtypeStruct((own, slots), F32),
        ),
        in_specs=[hbm] * 4,
        out_specs=(pl.BlockSpec(memory_space=pltpu.VMEM), pl.BlockSpec(memory_space=pltpu.VMEM)),
        scratch_shapes=[
            pltpu.VMEM((rows, width), BF16),
            pltpu.VMEM((rows, slots), BF16),
            pltpu.VMEM((rows, slots), F32),
            pltpu.VMEM((rows, slots), BF16),
            pltpu.VMEM((rows, slots), F32),
            pltpu.VMEM((PIECES, n, slots // n, width // PIECES), BF16),
            pltpu.VMEM((n, 2, own // 2, slots), BF16),
            pltpu.VMEM((n, 2, slots), F32),
            pltpu.VMEM((n, 1, slots), F32),
            pltpu.VMEM((4, 1, slots), F32),
            pltpu.VMEM((rows, slots), BF16),
            pltpu.VMEM((rows, slots), BF16),
            pltpu.VMEM((width, rows), BF16),
            pltpu.VMEM((2, 2, 2, half, quarter, slots), BF16),
            pltpu.VMEM((3, 2, half, quarter, slots), BF16),
            pltpu.VMEM((2, 2, 2, half, quarter, slots), F32),
            pltpu.VMEM((2, 2, 2, half, quarter, slots), BF16),
            pltpu.VMEM((2, 2, half, quarter, slots), BF16),
            pltpu.VMEM((2, 2, half, quarter, slots), F32),
            pltpu.VMEM((2, 2, half, quarter, slots), BF16),
            pltpu.VMEM((2, half, quarter, slots), BF16),
            pltpu.VMEM((n, quarter, slots), F32),
            pltpu.VMEM((2, half, quarter, slots), BF16),
            pltpu.VMEM((n, quarter, slots), BF16),
            pltpu.VMEM((4, quarter, slots), F32),
            dma((3 + PIECES,)),
            dma, dma((half, PIECES)), dma, dma((PIECES,)),
            dma, dma, dma, dma, dma, dma,
            dma, dma, dma, dma, dma, dma,
            dma, dma((2,)), dma, dma((2,)),
            dma, dma, dma, dma,
        ],
        compiler_params=pltpu.CompilerParams(
            collective_id=0, has_side_effects=True, vmem_limit_bytes=52_000_000
        ),
    )(*[
        pltpu.with_memory_space_constraint(x, pltpu.HBM)
        for x in (tokens, logits, slot_grad, phi_param.reshape(2, own // 2, slots))
    ])


def plain(tokens, logits, slot_grad, phi_param):
    inputs = tokens[0]
    scores = logits[0].astype(jnp.float32)
    upstream, phi_full = (
        lax.all_gather(slot_grad[0], "seq", axis=0, tiled=True),
        lax.all_gather(phi_param, "seq", axis=0, tiled=True),
    )
    weight_grad = lax.dot_general(
        inputs, upstream, (((1,), (1,)), ((), ())), preferred_element_type=jnp.float32
    )
    col_peak = lax.pmax(jnp.max(scores, axis=0, keepdims=True), "seq")
    raw_weights = jnp.exp(scores - col_peak)
    col_total = lax.psum(jnp.sum(raw_weights, axis=0, keepdims=True), "seq")
    dispatch = raw_weights / col_total
    col_dot = lax.psum(jnp.sum(dispatch * weight_grad, axis=0, keepdims=True), "seq")
    logit_grad = (dispatch * (weight_grad - col_dot)).astype(jnp.bfloat16)
    dispatch_low = dispatch.astype(jnp.bfloat16)
    grad_scale = float(lax.axis_size("seq") * inputs.shape[0] // 16)
    token_sum = jnp.dot(dispatch_low, upstream, preferred_element_type=jnp.float32)
    token_sum = token_sum + lax.dot_general(
        logit_grad, phi_full, (((1,), (1,)), ((), ())), preferred_element_type=jnp.float32
    )
    token_grad = (grad_scale * token_sum).astype(jnp.bfloat16)[None]
    phi_terms = lax.dot_general(
        inputs, logit_grad, (((0,), (0,)), ((), ())), preferred_element_type=jnp.float32
    )
    phi_share = lax.psum_scatter(phi_terms, "seq", scatter_dimension=0, tiled=True)
    phi_grad = lax.psum(phi_share, "batch")
    return (token_grad, phi_grad)


def per_device(n, batches, tokens, logits, slot_grad, phi_param):
    own, slots = phi_param.shape
    if batches == 4 and n % 8 == 0 and slot_grad.shape[1] % 16 == 0 and own % 128 == 0 and slots % 128 == 0 and tokens.shape[1] % 256 == 0:
        token_grad, phi_grad = fused(n, tokens[0], logits[0], slot_grad[0], phi_param)
        return token_grad[None], phi_grad
    return plain(tokens, logits, slot_grad, phi_param)


def solution(mesh):
    return jax.shard_map(
        functools.partial(per_device, mesh.shape["seq"], mesh.shape["batch"]),
        mesh=mesh,
        in_specs=(
            P("batch", "seq", None),
            P("batch", "seq", None),
            P("batch", "seq", None),
            P("seq", None),
        ),
        out_specs=(P("batch", "seq", None), P("seq", None)),
        check_vma=False,
    )
```

```python
import functools

import jax
import jax.numpy as jnp
from jax import lax
from jax.experimental import pallas as pl
from jax.experimental.pallas import tpu as pltpu
from jax.sharding import PartitionSpec as P

MESH = pl.DeviceIdType.MESH
F32 = jnp.float32
BF16 = jnp.bfloat16
PIECES = 2
LAG = 0.5
WGROWS = 512
CUTS = 4
LIMIT = 6_000_000
OUTROWS = 512


def fused_kernel(
    n, scale, tok_hbm, log_hbm, slot_hbm, phi_hbm, tok_out, phi_out,
    tok, log, raw, raw_low, wg, gath, phig, ends, dots, gam, disp, lg, tokt,
    mass, mass_in, part, part_low, recv_a, sum_a, low_a, recv_b, sum_b, low_b, recv_c, fin,
    load_sem, ag_send, ag_recv, fw_send, fw_recv, en_send, en_recv, do_send, do_recv, ga_send, ga_recv,
    ph_send, ph_recv, pa_send, pa_recv, m_send, m_recv,
    a_send, a_recv, b_send, b_recv, c_send, c_recv, d_send, d_recv,
):
    me = lax.axis_index("seq")
    bat = lax.axis_index("batch")
    half = n // 2
    place = me // 2
    col = me % 2
    twin = me + 1 - 2 * col
    bat_a = bat + 1 - 2 * (bat % 2)
    bat_b = (bat + 2) % 4
    bat_c = (bat_a + 2) % 4
    keep_a = bat % 2
    keep_b = bat // 2
    mates = ((bat_a, 1 - keep_a, keep_b), (bat_b, keep_a, 1 - keep_b), (bat_c, 1 - keep_a, 1 - keep_b))
    rows = tok.shape[0]
    slots = log.shape[1]
    step = min(256, rows)
    steps = rows // step
    large = min(WGROWS, rows)
    tall = min(OUTROWS, rows)
    pieces, span = gath.shape[0], gath.shape[3]
    own = tok.shape[1] // n
    quarter = own // 4
    group = n // 2
    owners = [[j for j in range(n) if (n // 4 <= j < n - n // 4) == bool(g)] for g in range(2)]

    def remote(src, dst, send, recv, seq_at, bat_at):
        return pltpu.make_async_remote_copy(
            src_ref=src, dst_ref=dst, send_sem=send, recv_sem=recv,
            device_id=(seq_at, bat_at), device_id_type=MESH,
        )

    def chunk(i):
        return pl.ds(pl.multiple_of(i * step, step), step)

    def wide(i):
        return pl.ds(pl.multiple_of(i * large, large), large)

    def band(i):
        return pl.ds(pl.multiple_of(i * tall, tall), tall)

    load_slot = [
        pltpu.make_async_copy(slot_hbm.at[:, q * span : (q + 1) * span], gath.at[q, me], load_sem.at[3 + q])
        for q in range(pieces)
    ]
    load_log = pltpu.make_async_copy(log_hbm, log, load_sem.at[0])
    load_phi = pltpu.make_async_copy(phi_hbm.at[keep_a], phig.at[me, keep_a], load_sem.at[1])
    load_tok = pltpu.make_async_copy(tok_hbm, tok, load_sem.at[2])
    for load in load_slot:
        load.start()
    load_log.start()
    load_tok.start()
    load_phi.start()

    barrier = pltpu.get_barrier_semaphore()
    for k in range(1, n):
        pl.semaphore_signal(barrier, inc=1, device_id=((me + k) % n, bat), device_id_type=MESH)
    for other in (bat_a, bat_b, bat_c):
        pl.semaphore_signal(barrier, inc=1, device_id=(me, other), device_id_type=MESH)
    pl.semaphore_wait(barrier, n - 1 + 3)

    def inside(p):
        return (p >= 0) & (p < half)

    def to_twin(p, q):
        shard = gath.at[q, 2 * p + col]
        return remote(shard, shard, fw_send, fw_recv.at[q], twin, bat)

    def along(p, target, q):
        shard = gath.at[q, 2 * p + col]
        return remote(shard, shard, ag_send, ag_recv.at[p, q], 2 * target + col, bat)

    def send_own():
        for q in range(pieces):
            load_slot[q].wait()
            to_twin(place, q).start()
            for dist in range(1, half):
                for sign in (1, -1):
                    @pl.when(inside(place + sign * dist))
                    def _(dist=dist, sign=sign, q=q):
                        along(place, place + sign * dist, q).start()

    def arrive(dist, sign, q):
        p = place + sign * dist

        @pl.when(inside(p))
        def _():
            along(p, p, q).wait_recv()
            to_twin(p, q).start()

    def whole(ref, sem):
        return remote(ref, ref, sem, sem, me, bat_a)

    @pl.when(keep_a == 0)
    def _():
        send_own()

    load_log.wait()

    def peak_step(i, top):
        return jnp.maximum(top, jnp.max(log[chunk(i), :].astype(F32), axis=0, keepdims=True))

    peak = lax.fori_loop(0, steps, peak_step, jnp.full((1, slots), -jnp.inf, F32))

    def exp_step(i, acc):
        values = jnp.exp(log[chunk(i), :].astype(F32) - peak)
        raw[chunk(i), :] = values
        raw_low[chunk(i), :] = values.astype(BF16)
        return acc + jnp.sum(values, axis=0, keepdims=True)

    total = lax.fori_loop(0, steps, exp_step, jnp.zeros((1, slots), F32))
    ends[me, 0:1, :] = peak
    ends[me, 1:2, :] = total
    for k in range(1, n):
        remote(ends.at[me], ends.at[me], en_send, en_recv, (me + k) % n, bat).start()

    @pl.when(keep_a == 1)
    def _():
        send_own()

    load_tok.wait()

    def turn_step(i, carry):
        tokt[:, chunk(i)] = tok[chunk(i), :].T
        return carry

    lax.fori_loop(0, steps, turn_step, 0)

    def terms_of(weights, g, at, put):
        j = owners[g][at]
        terms = jnp.dot(tokt[own * j : own * (j + 2), :], weights[...], preferred_element_type=F32)
        for side in range(2):
            for qa in range(2):
                for qb in range(2):
                    first = own * side + (2 * qa + qb) * quarter
                    put(g, qa, qb, at + side, terms[first : first + quarter, :])

    def put_mass(g, qa, qb, at, block):
        mass[g, qa, qb, at] = block.astype(BF16)


    def mass_task(g, at):
        terms_of(raw_low, g, at, put_mass)
        if at + 2 == group:
            for k, (mate, qa, qb) in enumerate(mates):
                remote(mass.at[g, qa, qb], mass_in.at[k, g], m_send, m_recv, me, mate).start()

    tasks = [(g, at) for g in range(2) for at in range(0, group, 2)]
    coming = sorted((q + LAG * (dist - 1), dist, q) for q in range(pieces) for dist in range(1, half))
    for _, dist, q in coming:
        if tasks:
            mass_task(*tasks.pop(0))
        for sign in (1, -1):
            arrive(dist, sign, q)
    for task in tasks:
        mass_task(*task)

    whole(ends.at[: n - 1], en_recv).wait_recv()
    peaks = ends[:, 0:1, :]
    col_peak = jnp.max(peaks, axis=0)
    col_total = jnp.sum(ends[:, 1:2, :] * jnp.exp(peaks - col_peak), axis=0)
    factor = jnp.exp(peak - col_peak) / col_total

    dot = jnp.zeros((1, slots), F32)
    for q in range(pieces):
        whole(gath.at[q, :half], fw_recv.at[q]).wait_recv()

        def wg_step(i, acc, q=q):
            values = lax.dot_general(
                tok[wide(i), q * span : (q + 1) * span], gath[q].reshape(slots, span),
                (((1,), (1,)), ((), ())), preferred_element_type=F32,
            )
            if q:
                values = values + wg[wide(i), :]
            wg[wide(i), :] = values
            if q == pieces - 1:
                acc = acc + jnp.sum(values * raw[wide(i), :], axis=0, keepdims=True)
            return acc

        dot = lax.fori_loop(0, rows // large, wg_step, dot)

    center = dot / total
    dots[me] = factor * dot
    gam[0, 0:1, :] = factor
    gam[0, 1:2, :] = center
    for k in range(1, n):
        remote(dots.at[me], dots.at[me], do_send, do_recv, (me + k) % n, bat).start()
    for k, (mate, _, _) in enumerate(mates):
        for other in range(n):
            remote(dots.at[me], dots.at[(1 + k) * n + me], do_send, do_recv, (me + other) % n, mate).start()
        remote(gam.at[0], gam.at[1 + k], ga_send, ga_recv, me, mate).start()
    load_phi.wait()
    for k in range(1, n):
        remote(phig.at[me, keep_a], phig.at[me, keep_a], ph_send, ph_recv, (me + k) % n, bat).start()

    def center_step(i, carry):
        lg[chunk(i), :] = (raw[chunk(i), :] * factor * (wg[chunk(i), :] - center)).astype(BF16)
        return carry

    lax.fori_loop(0, steps, center_step, 0)

    def put_part(g, qa, qb, at, block):
        part[g, qa, qb, at] = block
        part_low[g, qa, qb, at] = block.astype(BF16)

    moves_a = []
    for g in range(2):
        for at in range(0, group, 2):
            terms_of(lg, g, at, put_part)
        moves_a.append(remote(part_low.at[g, 1 - keep_a], recv_a.at[g], a_send, a_recv.at[g], me, bat_a))
        moves_a[-1].start()
    moves_b = []
    for g in range(2):
        moves_a[g].wait_recv()
        for qb in range(2):
            for at in range(group):
                block = part[g, keep_a, qb, at] + recv_a[g, qb, at].astype(F32)
                sum_a[g, qb, at] = block
                low_a[g, qb, at] = block.astype(BF16)
        moves_b.append(remote(low_a.at[g, 1 - keep_b], recv_b.at[g], b_send, b_recv.at[g], me, bat_b))
        moves_b[-1].start()

    whole(dots.at[: 4 * n - 1], do_recv).wait_recv()
    whole(gam.at[1:], ga_recv).wait_recv()
    col_dot = [jnp.sum(dots[k * n : (k + 1) * n], axis=0) for k in range(4)]
    shift = [gam[k, 0:1, :] * (gam[k, 1:2, :] - col_dot[k]) for k in range(4)]
    whole(mass_in, m_recv).wait_recv()

    def share_move(g, at):
        j = owners[g][at]
        return remote(low_b.at[g, at], recv_c.at[me], c_send, c_recv, j, bat)

    for g in range(2):
        moves_b[g].wait_recv()
        for at in range(group):
            block = sum_a[g, keep_b, at] + recv_b[g, at].astype(F32)
            block = block + mass[g, keep_a, keep_b, at].astype(F32) * shift[0]
            for k in range(3):
                block = block + mass_in[k, g, at].astype(F32) * shift[1 + k]
            sum_b[owners[g][at]] = block
            low_b[g, at] = block.astype(BF16)
        for at in range(group):
            @pl.when(me != owners[g][at])
            def _(g=g, at=at):
                share_move(g, at).start()

    whole(phig.at[: n - 1, 0], ph_recv).wait_recv()
    phi_a = remote(phig.at[:, keep_a], phig.at[:, keep_a], pa_send, pa_recv, me, bat_a)
    phi_a.start()

    def grad_step(i, carry):
        weights = raw[chunk(i), :] * factor
        grads = weights * (wg[chunk(i), :] - col_dot[0])
        disp[chunk(i), :] = weights.astype(BF16)
        lg[chunk(i), :] = grads.astype(BF16)
        return carry

    lax.fori_loop(0, steps, grad_step, 0)
    phi_a.wait_recv()
    phi_full = phig.reshape(n * own, slots)

    def out_step(i, carry):
        for q in range(pieces):
            values = jnp.dot(disp[band(i), :], gath[q].reshape(slots, span), preferred_element_type=F32)
            values = values + lax.dot_general(
                lg[band(i), :], phi_full[q * span : (q + 1) * span, :],
                (((1,), (1,)), ((), ())), preferred_element_type=F32,
            )
            tok_out[band(i), q * span : (q + 1) * span] = (scale * values).astype(BF16)
        return carry

    lax.fori_loop(0, rows // tall, out_step, 0)

    share = sum_b[me]
    whole(recv_c.at[: n - 1], c_recv).wait_recv()
    for k in range(1, n):
        share = share + recv_c[(me - k + n) % n].astype(F32)
    mine = 2 * keep_a + keep_b
    fin[mine] = share.astype(BF16)
    for k, other in enumerate((bat_c, bat_b, bat_a)):
        remote(fin.at[mine], fin.at[mine], d_send, d_recv, me, other).start()
    whole(fin.at[:3], d_recv).wait_recv()
    phi_out[...] = fin[...].astype(F32).reshape(own, slots)

    for ref, sem in (
        (gath.at[:, : half - 1], ag_send), (gath.at[:, :half], fw_send), (ends.at[: n - 1], en_send), (dots.at[: 4 * n - 1], do_send),
        (gam.at[1:], ga_send), (phig.at[: n - 1, 0], ph_send), (phig.at[:, 0], pa_send), (mass_in, m_send),
        (recv_a, a_send), (recv_b, b_send), (recv_c.at[: n - 1], c_send), (fin.at[:3], d_send),
    ):
        whole(ref, sem).wait_send()


def place_kernel(tok_in, phi_in, tok_hbm, phi_hbm, sem):
    block = tok_in.shape[0] // CUTS
    moves = [pltpu.make_async_copy(phi_in, phi_hbm, sem.at[CUTS])]
    for k in range(CUTS):
        part = pl.ds(k * block, block)
        moves.append(pltpu.make_async_copy(tok_in.at[part], tok_hbm.at[part], sem.at[k]))
    for move in moves:
        move.start()
    for move in moves:
        move.wait()


def fused(n, tokens, logits, slot_grad, phi_param):
    rows, width = tokens.shape
    slots = logits.shape[1]
    own = width // n
    quarter = own // 4
    half = n // 2
    scale = float(n * rows // 16)
    dma = pltpu.SemaphoreType.DMA
    hbm = pl.BlockSpec(memory_space=pltpu.HBM)
    grads = pl.pallas_call(
        functools.partial(fused_kernel, n, scale),
        out_shape=(
            jax.ShapeDtypeStruct((rows, width), BF16),
            jax.ShapeDtypeStruct((own, slots), F32),
        ),
        in_specs=[hbm] * 4,
        out_specs=(pl.BlockSpec(memory_space=pltpu.VMEM), pl.BlockSpec(memory_space=pltpu.VMEM)),
        scratch_shapes=[
            pltpu.VMEM((rows, width), BF16),
            pltpu.VMEM((rows, slots), BF16),
            pltpu.VMEM((rows, slots), F32),
            pltpu.VMEM((rows, slots), BF16),
            pltpu.VMEM((rows, slots), F32),
            pltpu.VMEM((PIECES, n, slots // n, width // PIECES), BF16),
            pltpu.VMEM((n, 2, own // 2, slots), BF16),
            pltpu.VMEM((n, 2, slots), F32),
            pltpu.VMEM((4 * n, 1, slots), F32),
            pltpu.VMEM((4, 2, slots), F32),
            pltpu.VMEM((rows, slots), BF16),
            pltpu.VMEM((rows, slots), BF16),
            pltpu.VMEM((width, rows), BF16),
            pltpu.VMEM((2, 2, 2, half, quarter, slots), BF16),
            pltpu.VMEM((3, 2, half, quarter, slots), BF16),
            pltpu.VMEM((2, 2, 2, half, quarter, slots), F32),
            pltpu.VMEM((2, 2, 2, half, quarter, slots), BF16),
            pltpu.VMEM((2, 2, half, quarter, slots), BF16),
            pltpu.VMEM((2, 2, half, quarter, slots), F32),
            pltpu.VMEM((2, 2, half, quarter, slots), BF16),
            pltpu.VMEM((2, half, quarter, slots), BF16),
            pltpu.VMEM((n, quarter, slots), F32),
            pltpu.VMEM((2, half, quarter, slots), BF16),
            pltpu.VMEM((n, quarter, slots), BF16),
            pltpu.VMEM((4, quarter, slots), BF16),
            dma((3 + PIECES,)),
            dma, dma((half, PIECES)), dma, dma((PIECES,)),
            dma, dma, dma, dma, dma, dma,
            dma, dma, dma, dma, dma, dma,
            dma, dma((2,)), dma, dma((2,)),
            dma, dma, dma, dma,
        ],
        compiler_params=pltpu.CompilerParams(
            collective_id=0, has_side_effects=True, vmem_limit_bytes=52_000_000
        ),
    )(*[
        pltpu.with_memory_space_constraint(x, pltpu.HBM)
        for x in (tokens, logits, slot_grad, phi_param.reshape(2, own // 2, slots))
    ])
    return pl.pallas_call(
        place_kernel,
        out_shape=(
            jax.ShapeDtypeStruct((rows, width), BF16),
            jax.ShapeDtypeStruct((own, slots), F32),
        ),
        in_specs=[pl.BlockSpec(memory_space=pltpu.VMEM)] * 2,
        out_specs=(hbm, hbm),
        scratch_shapes=[dma((CUTS + 1,))],
        compiler_params=pltpu.CompilerParams(vmem_limit_bytes=LIMIT),
    )(*grads)


def plain(tokens, logits, slot_grad, phi_param):
    inputs = tokens[0]
    scores = logits[0].astype(jnp.float32)
    upstream, phi_full = (
        lax.all_gather(slot_grad[0], "seq", axis=0, tiled=True),
        lax.all_gather(phi_param, "seq", axis=0, tiled=True),
    )
    weight_grad = lax.dot_general(
        inputs, upstream, (((1,), (1,)), ((), ())), preferred_element_type=jnp.float32
    )
    col_peak = lax.pmax(jnp.max(scores, axis=0, keepdims=True), "seq")
    raw_weights = jnp.exp(scores - col_peak)
    col_total = lax.psum(jnp.sum(raw_weights, axis=0, keepdims=True), "seq")
    dispatch = raw_weights / col_total
    col_dot = lax.psum(jnp.sum(dispatch * weight_grad, axis=0, keepdims=True), "seq")
    logit_grad = (dispatch * (weight_grad - col_dot)).astype(jnp.bfloat16)
    dispatch_low = dispatch.astype(jnp.bfloat16)
    grad_scale = float(lax.axis_size("seq") * inputs.shape[0] // 16)
    token_sum = jnp.dot(dispatch_low, upstream, preferred_element_type=jnp.float32)
    token_sum = token_sum + lax.dot_general(
        logit_grad, phi_full, (((1,), (1,)), ((), ())), preferred_element_type=jnp.float32
    )
    token_grad = (grad_scale * token_sum).astype(jnp.bfloat16)[None]
    phi_terms = lax.dot_general(
        inputs, logit_grad, (((0,), (0,)), ((), ())), preferred_element_type=jnp.float32
    )
    phi_share = lax.psum_scatter(phi_terms, "seq", scatter_dimension=0, tiled=True)
    phi_grad = lax.psum(phi_share, "batch")
    return (token_grad, phi_grad)


def per_device(n, batches, tokens, logits, slot_grad, phi_param):
    own, slots = phi_param.shape
    if batches == 4 and n % 8 == 0 and slot_grad.shape[1] % 16 == 0 and own % 128 == 0 and slots % 128 == 0 and tokens.shape[1] % 256 == 0:
        token_grad, phi_grad = fused(n, tokens[0], logits[0], slot_grad[0], phi_param)
        return token_grad[None], phi_grad
    return plain(tokens, logits, slot_grad, phi_param)


def solution(mesh):
    return jax.shard_map(
        functools.partial(per_device, mesh.shape["seq"], mesh.shape["batch"]),
        mesh=mesh,
        in_specs=(
            P("batch", "seq", None),
            P("batch", "seq", None),
            P("batch", "seq", None),
            P("seq", None),
        ),
        out_specs=(P("batch", "seq", None), P("seq", None)),
        check_vma=False,
    )
```
